32 devices in a mesh: tensor: 8 (over z, y), dp: 4 (over x, core).
Axes of the slice: x: 2, y: 2, z: 4, core: 2. Of those that a mesh axis runs over, the one named last changes fastest.
Arguments:
- base_weight: bfloat16 [2, 2, 4096, 14336], P(None, None, 'tensor', 'dp'), may hold values from -0.125 to 0.125
- adapter_left: bfloat16 [2, 2, 4096, 16], P(None, None, 'tensor'), may hold values from -0.059814453 to 0.059814453
- adapter_right: bfloat16 [2, 2, 16, 14336], P(None, None, None, 'dp'), may hold values from -1.5 to 1.5
- magnitude: bfloat16 [2, 2, 14336], P(None, None, 'dp'), may hold values from 16 to 256
Outputs:
- merged_weight: bfloat16 [2, 2, 14336, 4096], P(None, None, 'tensor')
The draws below stay inside these ranges and needn't reach their ends.
All inputs are finite; a program needn't handle non-finite values.
Results may differ from the reference program's by a relative error of at most 0.0004.
Values may be sent and summed in bfloat16 or wider, within the bound.
A program may use at most 384 MiB of HBM per device.

```python
import math
import jax
import jax.numpy as jnp
from jax import lax

D = 4096
FF = 14336
RANK = 16
EXP = 2
PROJ = 2


def with_spikes(result, key, source, target, blocks, factor):
    def block_of(axis_at):
        return (jnp.arange(result.shape[axis_at]) // (result.shape[axis_at] // blocks)).reshape((-1,) + (1,) * (result.ndim - 1 - axis_at))

    first = jax.random.permutation(key, blocks)[block_of(target)]
    second = (block_of(target) + blocks // 2) % blocks
    return jnp.where((block_of(source) == first) | (block_of(source) == second), factor * result, result)


def block_scale(key, shape, pieces, low, high):
    def one(dim, parts):
        heights = jax.random.uniform(jax.random.fold_in(jax.random.fold_in(key, 6), dim), (parts,), jnp.float32, low / len(pieces), high / len(pieces))
        return jnp.repeat(jnp.exp(heights), shape[dim] // parts).reshape((-1,) + (1,) * (len(shape) - dim - 1))

    level = one(*pieces[0])
    for cut in pieces[1:]:
        level = level * one(*cut)
    return level


def noise(rng, extent, scale, bound, cuts=(), dtype=jnp.bfloat16):
    entries = scale * jax.random.normal(rng, extent, jnp.float32)
    if cuts:
        entries = entries * block_scale(rng, extent, cuts, -0.22, 0.18)
    return jnp.clip(entries, -bound, bound).astype(dtype)


def bell_draw_with(stream_key, extent, deviation, most, pieces, heavy, kind=jnp.bfloat16):
    drawn = deviation * jax.random.normal(stream_key, extent, jnp.float32)
    if pieces:
        drawn = drawn * block_scale(stream_key, extent, pieces, -0.22, 0.18)
    return jnp.clip(with_spikes(drawn, jax.random.fold_in(stream_key, 3), *heavy), -most, most).astype(kind)


def setup_inputs(seed: int = 0) -> dict:
    key_of = jax.random.split(jax.random.key(seed), 5)
    return {
        "base_weight": bell_draw_with(key_of[0], (EXP, PROJ, D, FF), D ** -0.5, 0.125, ((2, 8), (3, 4)), (2, 3, 8, 2.0)),
        "adapter_left": noise(key_of[1], (EXP, PROJ, D, RANK), 0.01, 0.059814453, ((2, 8),)),
        "adapter_right": noise(key_of[2], (EXP, PROJ, RANK, FF), RANK ** -0.5, 1.5, ((3, 4),)),
        "magnitude": jnp.clip(jnp.exp(math.log(256.0) - 2.7725887 * jax.random.uniform(key_of[3], (EXP, PROJ, FF), jnp.float32) ** block_scale(key_of[3], (EXP, PROJ, FF), ((2, 4),), -0.2, 0.2)), 16.0, 256.0).astype(jnp.bfloat16),
    }


def merge_one(operands):
    weight, left_factor, right_factor, column_scale = operands
    merged = weight.astype(jnp.float32) + jnp.dot(left_factor, right_factor, preferred_element_type=jnp.float32)
    squares = lax.optimization_barrier(jnp.sum(merged * merged, axis=0))
    scaling = column_scale.astype(jnp.float32) / jnp.sqrt(squares + 1e-06)
    return (merged * scaling[None, :]).astype(jnp.bfloat16).T

def reference(base_weight, adapter_left, adapter_right, magnitude):
    stacked = lax.map(merge_one, (base_weight.reshape(EXP * PROJ, D, FF), adapter_left.reshape(EXP * PROJ, D, RANK), adapter_right.reshape(EXP * PROJ, RANK, FF), magnitude.reshape(EXP * PROJ, FF)))
    return stacked.reshape(EXP, PROJ, FF, D)
```

```python
import functools

import jax
import jax.numpy as jnp
from jax import lax
from jax.experimental import pallas as pl
from jax.experimental.pallas import tpu as pltpu
from jax.sharding import PartitionSpec as P

MESH = pl.DeviceIdType.MESH


def exchange_kernel(sizes, chunks, relayed, s, g, rb, recv, xs, cs, a_send, a_recv, b_send, r_send):
    tensor_count, replica_count = sizes
    group = tensor_count // replica_count
    half_t, half_r = tensor_count // 2, replica_count // 2
    serve = s.shape[3]
    parts = ((0, relayed), (relayed, serve - relayed))
    t, d = lax.axis_index("tensor"), lax.axis_index("dp")
    twin = lax.rem(d + half_r, replica_count)
    mate = d + 1 - 2 * lax.rem(d, 2)
    near = t // half_t == d // half_r
    far = jnp.logical_not(near)
    home = t // group
    is_home, is_twin = home == d, home == twin
    base = (t // half_t) * half_t
    other = half_t - base

    def near_source(i):
        return base + lax.rem(t - base + i, half_t)

    def far_source(i):
        return other + lax.rem(t - base + i, half_t)

    def own(k, j, p):
        return s.at[k, j, :, pl.ds(*parts[p])]

    def slot(ts, k, p):
        return g.at[ts, k, :, pl.ds(*parts[p])]

    def send(src, ts, k, p, sem, tensor, dp):
        return pltpu.make_async_remote_copy(
            src_ref=src, dst_ref=slot(ts, k, p), send_sem=sem, recv_sem=recv.at[ts, k, p],
            device_id={"tensor": tensor, "dp": dp}, device_id_type=MESH,
        )

    def to_twin(src, ts, k, p):
        return send(src, ts, k, p, xs.at[ts, k, p], t, twin)

    def to_mate(src, ts, k, p):
        return send(src, ts, k, p, cs.at[ts, k, p], t, mate)

    def to_relay(k, j):
        return pltpu.make_async_remote_copy(
            src_ref=own(k, j, 0), dst_ref=rb.at[k, j], send_sem=a_send.at[k, j], recv_sem=a_recv.at[k, j],
            device_id={"tensor": t, "dp": twin}, device_id_type=MESH,
        )

    def relay(k, j):
        return send(rb.at[k, j], t, k, 0, r_send.at[k, j], twin * group + j, d)

    def direct(k, j, p):
        return send(own(k, j, p), t, k, p, b_send.at[k, j, p], d * group + j, d)

    def keep(k, p):
        return pltpu.make_async_copy(own(k, lax.rem(t, group), p), slot(t, k, p), recv.at[t, k, p])

    def got(ts, k, p):
        to_mate(slot(ts, k, p), ts, k, p).wait_recv()

    def loop(count, body, first=0):
        lax.fori_loop(first, count, lambda i, c: (body(i), c)[1], 0)

    def each_piece(body):
        loop(chunks, lambda k: loop(group, lambda j: body(k, j)))

    def start_piece(k, j):
        leaves = d * group + j != t

        @pl.when(far)
        def _():
            to_relay(k, j).start()
            direct(k, j, 1).start()

        @pl.when(jnp.logical_and(near, leaves))
        def _():
            direct(k, j, 0).start()
            direct(k, j, 1).start()

        @pl.when(jnp.logical_not(leaves))
        def _():
            for p in range(2):
                src = own(k, j, p)
                to_twin(src, t, k, p).start()
                to_mate(src, t, k, p).start()
                keep(k, p).start()

    each_piece(start_piece)

    def pass_on(ts, k, p):
        got(ts, k, p)
        to_twin(slot(ts, k, p), ts, k, p).start()
        to_mate(slot(ts, k, p), ts, k, p).start()

    def hand_over(ts, k, p):
        got(ts, k, p)
        to_mate(slot(ts, k, p), ts, k, p).start()

    def relay_step(k):
        @pl.when(near)
        def _():
            def one(j):
                to_relay(k, j).wait_recv()
                relay(k, j).start()

            loop(group, one)

    def arrivals(k):
        @pl.when(is_home)
        def _():
            def one(i):
                pass_on(near_source(i), k, 0)
                pass_on(near_source(i), k, 1)

            loop(half_t, one, 1)
            loop(half_t, lambda i: pass_on(far_source(i), k, 1))

        @pl.when(is_twin)
        def _():
            loop(half_t, lambda i: pass_on(far_source(i), k, 0))

    def second_hand(k):
        @pl.when(is_home)
        def _():
            loop(half_t, lambda i: hand_over(far_source(i), k, 0))

        @pl.when(is_twin)
        def _():
            def one(i):
                hand_over(near_source(i), k, 0)
                hand_over(near_source(i), k, 1)

            loop(half_t, one)
            loop(half_t, lambda i: hand_over(far_source(i), k, 1))

    relay_step(0)

    def step(k):
        @pl.when(k + 1 < chunks)
        def _():
            relay_step(k + 1)

        arrivals(k)

        @pl.when(k > 0)
        def _():
            second_hand(k - 1)

    loop(chunks, step)
    second_hand(chunks - 1)

    serving = jnp.logical_or(is_home, is_twin)

    @pl.when(jnp.logical_not(serving))
    def _():
        def one(k, ts):
            got(ts, k, 0)
            got(ts, k, 1)

        loop(chunks, lambda k: loop(tensor_count, lambda ts: one(k, ts)))

    @pl.when(is_home)
    def _():
        def one(k):
            keep(k, 0).wait()
            keep(k, 1).wait()

        loop(chunks, one)

    def finish_piece(k, j):
        leaves = d * group + j != t

        @pl.when(far)
        def _():
            to_relay(k, j).wait_send()
            direct(k, j, 1).wait_send()

        @pl.when(near)
        def _():
            relay(k, j).wait_send()

        @pl.when(jnp.logical_and(near, leaves))
        def _():
            direct(k, j, 0).wait_send()
            direct(k, j, 1).wait_send()

    each_piece(finish_piece)

    @pl.when(serving)
    def _():
        def one(k, ts):
            to_mate(slot(ts, k, 0), ts, k, 0).wait_send()
            to_mate(slot(ts, k, 1), ts, k, 1).wait_send()

        loop(chunks, lambda k: loop(tensor_count, lambda ts: one(k, ts)))

    @pl.when(is_home)
    def _():
        def one(k, i):
            to_twin(slot(near_source(i), k, 0), near_source(i), k, 0).wait_send()
            to_twin(slot(near_source(i), k, 1), near_source(i), k, 1).wait_send()
            to_twin(slot(far_source(i), k, 1), far_source(i), k, 1).wait_send()

        loop(chunks, lambda k: loop(half_t, lambda i: one(k, i)))

    @pl.when(is_twin)
    def _():
        def one(k, i):
            to_twin(slot(far_source(i), k, 0), far_source(i), k, 0).wait_send()

        loop(chunks, lambda k: loop(half_t, lambda i: one(k, i)))


def exchange(s, tensor_count, replica_count, relayed):
    chunks, group, each, serve, rows = s.shape
    dma = pltpu.SemaphoreType.DMA
    g, _ = pl.pallas_call(
        functools.partial(exchange_kernel, (tensor_count, replica_count), chunks, relayed),
        out_shape=(
            jax.ShapeDtypeStruct((tensor_count, chunks, each, serve, rows), s.dtype),
            jax.ShapeDtypeStruct((chunks, group, each, relayed, rows), s.dtype),
        ),
        in_specs=[pl.BlockSpec(memory_space=pl.ANY)],
        out_specs=[pl.BlockSpec(memory_space=pl.ANY)] * 2,
        scratch_shapes=[dma((tensor_count, chunks, 2))] * 3
        + [dma((chunks, group))] * 2
        + [dma((chunks, group, 2)), dma((chunks, group))],
        compiler_params=pltpu.CompilerParams(has_side_effects=True),
    )(s)
    return g


def flip_kernel(w, o):
    o[0] = w[0].T


def flip(w):
    stacks, rows, cols = w.shape
    if rows % 128:
        return w.swapaxes(1, 2)
    wide = next(n for n in (512, 256, 128, cols) if cols % n == 0)
    return pl.pallas_call(
        flip_kernel,
        grid=(stacks, cols // wide),
        in_specs=[pl.BlockSpec((1, rows, wide), lambda e, c: (e, 0, c))],
        out_specs=pl.BlockSpec((1, wide, rows), lambda e, c: (e, c, 0)),
        out_shape=jax.ShapeDtypeStruct((stacks, cols, rows), w.dtype),
    )(w)


def merge_kernel(count, rows, g, left, right, magnitude, o, merged):
    squares = None
    for n in range(count):
        at = slice(n * rows, (n + 1) * rows)
        piece = g[n, 0].astype(jnp.float32) + jnp.dot(
            right[0], left[0, :, at], preferred_element_type=jnp.float32
        )
        merged[:, at] = piece
        total = jnp.sum(piece * piece, axis=1, keepdims=True)
        squares = total if squares is None else squares + total
    scaling = magnitude[0].astype(jnp.float32) / jnp.sqrt(squares + 1e-06)
    for n in range(count):
        at = slice(n * rows, (n + 1) * rows)
        o[0, :, at] = (merged[:, at] * scaling).astype(o.dtype)


def merge(g, left, right, magnitude):
    count, stacks, serve, rows = g.shape
    rank = right.shape[2]
    if rows % 128:
        joined = g.transpose(1, 2, 0, 3).reshape(stacks, serve, count * rows)
        merged = joined.astype(jnp.float32) + jnp.einsum(
            "xfr,xri->xfi", right, left, preferred_element_type=jnp.float32
        )
        squares = jnp.sum(merged * merged, axis=2, keepdims=True)
        scaling = magnitude.astype(jnp.float32) / jnp.sqrt(squares + 1e-06)
        return (merged * scaling).astype(g.dtype)
    tall = next(n for n in (256, 128, 64, 32, 16, serve) if serve % n == 0)
    return pl.pallas_call(
        functools.partial(merge_kernel, count, rows),
        grid=(stacks, serve // tall),
        in_specs=[
            pl.BlockSpec((count, 1, tall, rows), lambda e, f: (0, e, f, 0)),
            pl.BlockSpec((1, rank, count * rows), lambda e, f: (e, 0, 0)),
            pl.BlockSpec((1, tall, rank), lambda e, f: (e, f, 0)),
            pl.BlockSpec((1, tall, 1), lambda e, f: (e, f, 0)),
        ],
        out_specs=pl.BlockSpec((1, tall, count * rows), lambda e, f: (e, f, 0)),
        out_shape=jax.ShapeDtypeStruct((stacks, serve, count * rows), g.dtype),
        scratch_shapes=[pltpu.VMEM((tall, count * rows), jnp.float32)],
    )(g, left, right, magnitude)


UNIT = 128
AHEAD, RELAY_AHEAD, MERGE_LAG = 4, 2, 1


def fused_kernel(
    tensor_count, w, lt, r, m, o, s, g, rb, win, left, right, strength, merged, ob,
    w_sem, s_send, g_recv, rb_recv, rb_send, f_send, l_own, l_recv, l_send, l_mate, l_twin,
    p_recv, p_send, o_local, o_send, o_recv,
):
    units, _, unit, rows = g.shape
    group = s.shape[1]
    half_t = tensor_count // 2
    serve = o.shape[1]
    half = serve // 2
    per = half // unit
    stacks = units // per
    t, d = lax.axis_index("tensor"), lax.axis_index("dp")
    x, c = d // 2, lax.rem(d, 2)
    twin = lax.rem(d + 2, 4)
    mate = d + 1 - 2 * c
    near = t // half_t == x
    far = jnp.logical_not(near)
    home = t // group == d
    base = (t // half_t) * half_t
    other = half_t - base

    def near_source(i):
        return base + lax.rem(t - base + i, half_t)

    def far_source(i):
        return other + lax.rem(t - base + i, half_t)

    def loop(count, body, first=0):
        lax.fori_loop(first, count, lambda i, carry: (body(i), carry)[1], 0)

    def is_direct(v, h):
        return lax.rem(v + h, 3) == 1

    def direct_before(v, h):
        return (v + 1 + h) // 3

    def relay_index(v, h):
        return v - direct_before(v, h)

    def remote(src, dst, send_sem, recv_sem, tensor, dp):
        return pltpu.make_async_remote_copy(
            src_ref=src, dst_ref=dst, send_sem=send_sem, recv_sem=recv_sem,
            device_id={"tensor": tensor, "dp": dp}, device_id_type=MESH,
        )

    pairs = [(j, h) for j in range(group) for h in range(2)]

    def load(v, j, h):
        k, q = v // per, lax.rem(v, per)
        at = pl.multiple_of(j * serve + h * half + q * unit, unit)
        slot = lax.rem(v, 2)
        return pltpu.make_async_copy(
            w.at[k, :, pl.ds(at, unit)], win.at[slot, j, h], w_sem.at[slot, j, h]
        )

    def start_load(v):
        for j, h in pairs:
            load(v, j, h).start()

    def to_server(v, j, h):
        return remote(
            s.at[v, j, h], g.at[v, t], s_send.at[v // per, j, h], g_recv.at[v, t],
            d * group + j, x * 2 + h,
        )

    def to_relay(v, j, h):
        at = relay_index(v, h)
        return remote(
            s.at[v, j, h], rb.at[at, j, h], s_send.at[v // per, j, h], rb_recv.at[at, j, h], t, twin
        )

    def stays(j, h):
        return jnp.logical_and(d * group + j == t, c == h)

    def flip_and_send(v):
        slot = lax.rem(v, 2)
        for j, h in pairs:
            load(v, j, h).wait()
            turned = win[slot, j, h].T
            s[v, j, h] = turned
            own = stays(j, h)

            @pl.when(own)
            def _():
                g[v, t] = turned

            by_hand = jnp.logical_and(far, jnp.logical_not(is_direct(v, h)))

            @pl.when(by_hand)
            def _():
                to_relay(v, j, h).start()

            @pl.when(jnp.logical_not(jnp.logical_or(own, by_hand)))
            def _():
                to_server(v, j, h).start()

        @pl.when(v + 2 < units)
        def _():
            start_load(v + 2)

    def relay(v, j, h):
        return remote(
            rb.at[relay_index(v, h), j, h], g.at[v, t], rb_send.at[j, h], g_recv.at[v, t],
            twin * group + j, x * 2 + h,
        )

    def relay_step(v):
        for j, h in pairs:

            @pl.when(jnp.logical_and(near, jnp.logical_not(is_direct(v, h))))
            def _():
                to_relay(v, j, h).wait_recv()
                relay(v, j, h).start()

    def forward(v, ts):
        return remote(g.at[v, ts], g.at[v, ts], f_send.at[ts], g_recv.at[v, ts], t, twin)

    def got(v, ts):
        forward(v, ts).wait_recv()

    def pass_on(v, ts):
        got(v, ts)
        forward(v, ts).start()

    def arrivals(v):
        @pl.when(near)
        def _():
            @pl.when(home)
            def _():
                forward(v, t).start()

            @pl.when(jnp.logical_not(home))
            def _():
                pass_on(v, t)

            loop(half_t, lambda i: pass_on(v, near_source(i)), 1)

            @pl.when(is_direct(v, c))
            def _():
                loop(half_t, lambda i: pass_on(v, far_source(i)))

        @pl.when(jnp.logical_and(far, jnp.logical_not(is_direct(v, c))))
        def _():
            loop(half_t, lambda i: pass_on(v, far_source(i)))

    def second_hand(v):
        @pl.when(far)
        def _():
            loop(half_t, lambda i: got(v, near_source(i)))

            @pl.when(is_direct(v, c))
            def _():
                loop(half_t, lambda i: got(v, far_source(i)))

        @pl.when(jnp.logical_and(near, jnp.logical_not(is_direct(v, c))))
        def _():
            loop(half_t, lambda i: got(v, far_source(i)))

    def out_rows(v, core):
        k, q = v // per, lax.rem(v, per)
        return o.at[k, pl.ds(pl.multiple_of(core * half + q * unit, unit), unit)]

    def out_local(v):
        slot = lax.rem(v, 2)
        return pltpu.make_async_copy(ob.at[slot], out_rows(v, c), o_local.at[slot])

    def out_mate(v):
        slot = lax.rem(v, 2)
        return remote(ob.at[slot], out_rows(v, c), o_send.at[slot], o_recv.at[v // per], t, mate)

    def merge_unit(v):
        k, q = v // per, lax.rem(v, per)
        slot = lax.rem(v, 2)
        lanes = pl.ds(pl.multiple_of(q * unit, unit), unit)
        second_hand(v)
        factor = right[k, :, lanes]
        squares = jnp.zeros((unit, 128), jnp.float32)
        for n in range(tensor_count):
            piece = g[v, n].astype(jnp.float32) + lax.dot_general(
                factor, left[n, k], (((0,), (0,)), ((), ())), preferred_element_type=jnp.float32
            )
            merged[:, n * rows : (n + 1) * rows] = piece
            for b in range(rows // 128):
                part = piece[:, b * 128 : (b + 1) * 128]
                squares = squares + part * part
        total = jnp.sum(squares, axis=1, keepdims=True)
        stack = lax.broadcasted_iota(jnp.int32, (stacks, unit), 0)
        chosen = jnp.sum(jnp.where(stack == k, strength[:, lanes], 0.0), axis=0, keepdims=True)
        wide = jnp.broadcast_to(chosen, (unit, unit)).T
        scaling = wide / jnp.sqrt(total + 1e-06)

        @pl.when(v >= 2)
        def _():
            out_local(v - 2).wait()
            out_mate(v - 2).wait_send()

        for b in range(tensor_count * rows // 128):
            at = slice(b * 128, (b + 1) * 128)
            ob[slot, :, at] = (merged[:, at] * scaling).astype(ob.dtype)
        out_local(v).start()
        out_mate(v).start()

    carrier = lax.rem(t, 2) == c

    def left_out(ts):
        return remote(lt, left.at[t], l_send.at[ts], l_recv.at[t], ts, d)

    def left_mate(ts):
        return remote(left.at[ts], left.at[ts], l_mate.at[ts], l_recv.at[ts], t, mate)

    def left_twin(ts):
        return remote(left.at[ts], left.at[ts], l_twin.at[ts], l_recv.at[ts], t, twin)

    own_left = pltpu.make_async_copy(lt, left.at[t], l_own)

    def factors(h, dp):
        at = pl.multiple_of(lax.rem(t, group) * serve + h * half, unit)
        way = dp // 2
        return (
            remote(r.at[:, :, pl.ds(at, half)], right, p_send.at[0, way, h], p_recv.at[0], t, dp),
            remote(m.at[:, pl.ds(at, half)], strength, p_send.at[1, way, h], p_recv.at[1], t, dp),
        )

    def own_factors(h):
        at = pl.multiple_of(lax.rem(t, group) * serve + h * half, unit)
        return (
            pltpu.make_async_copy(r.at[:, :, pl.ds(at, half)], right, p_recv.at[0]),
            pltpu.make_async_copy(m.at[:, pl.ds(at, half)], strength, p_recv.at[1]),
        )

    def each_factor(remote_do, own_do):
        for way in range(2):
            for h in range(2):
                dp = way * 2 + h

                if remote_do:

                    @pl.when(jnp.logical_and(home, d != dp))
                    def _():
                        for copy in factors(h, dp):
                            remote_do(copy)

                if own_do:

                    @pl.when(jnp.logical_and(home, d == dp))
                    def _():
                        for copy in own_factors(h):
                            own_do(copy)

    start_load(0)
    start_load(1)
    own_left.start()
    flip_and_send(0)

    @pl.when(carrier)
    def _():
        loop(half_t, lambda i: left_out(near_source(i)).start(), 1)

        @pl.when(far)
        def _():
            loop(half_t, lambda i: left_out(far_source(i)).start())

    each_factor(lambda copy: copy.start(), lambda copy: copy.start())
    loop(AHEAD, flip_and_send, 1)
    loop(RELAY_AHEAD, relay_step)

    def spread_left(ts, across):
        left_mate(ts).wait_recv()

        @pl.when(lax.rem(ts, 2) == c)
        def _():
            left_mate(ts).start()
            if across:

                @pl.when(near)
                def _():
                    left_twin(ts).start()

    loop(half_t, lambda i: spread_left(near_source(i), False), 1)
    loop(half_t, lambda i: spread_left(far_source(i), True))
    own_left.wait()

    @pl.when(jnp.logical_not(home))
    def _():
        for copy in factors(0, mate):
            copy.wait_recv()

    each_factor(None, lambda copy: copy.wait())

    def step(v):
        @pl.when(v + AHEAD < units)
        def _():
            flip_and_send(v + AHEAD)

        @pl.when(v + RELAY_AHEAD < units)
        def _():
            relay_step(v + RELAY_AHEAD)

        arrivals(v)

        @pl.when(v >= MERGE_LAG)
        def _():
            merge_unit(v - MERGE_LAG)

    loop(units, step)
    loop(units, merge_unit, units - MERGE_LAG)

    for v in (units - 2, units - 1):
        out_local(v).wait()
        out_mate(v).wait_send()
    for k in range(stacks):
        rows_in = o.at[k, pl.ds(pl.multiple_of((1 - c) * half, unit), half)]
        remote(rows_in, rows_in, o_send.at[0], o_recv.at[k], t, mate).wait_recv()
    for k in range(stacks):
        for j, h in pairs:

            @pl.when(jnp.logical_not(stays(j, h)))
            def _():
                sent = s.at[k * per : (k + 1) * per, j, h]
                remote(sent, sent, s_send.at[k, j, h], g_recv.at[0, 0], t, twin).wait_send()

    @pl.when(near)
    def _():
        for j, h in pairs:
            sent = rb.at[0 : units - (units + 1 + h) // 3, j, h]
            remote(sent, sent, rb_send.at[j, h], g_recv.at[0, 0], t, twin).wait_send()

    def sent_on(ts, count):
        sent = g.at[0:count, ts]
        remote(sent, sent, f_send.at[ts], g_recv.at[0, 0], t, twin).wait_send()

    @pl.when(near)
    def _():
        loop(half_t, lambda i: sent_on(near_source(i), units))

    for h in range(2):
        count = (units + 1 + h) // 3

        @pl.when(jnp.logical_and(near, c == h))
        def _():
            loop(half_t, lambda i: sent_on(far_source(i), count))

        @pl.when(jnp.logical_and(far, c == h))
        def _():
            loop(half_t, lambda i: sent_on(far_source(i), units - count))

    @pl.when(carrier)
    def _():
        loop(half_t, lambda i: left_out(near_source(i)).wait_send(), 1)

        @pl.when(far)
        def _():
            loop(half_t, lambda i: left_out(far_source(i)).wait_send())

    def left_sent(ts, across):
        @pl.when(lax.rem(ts, 2) == c)
        def _():
            left_mate(ts).wait_send()
            if across:

                @pl.when(near)
                def _():
                    left_twin(ts).wait_send()

    loop(half_t, lambda i: left_sent(near_source(i), False), 1)
    loop(half_t, lambda i: left_sent(far_source(i), True))
    each_factor(lambda copy: copy.wait_send(), None)


def fused(w, lt, r, m, tensor_count):
    stacks, rows, cols = w.shape
    rank = lt.shape[1]
    group = tensor_count // 4
    serve = cols // group
    half = serve // 2
    per = half // UNIT
    units = stacks * per
    relayed = units - (units + 1) // 3
    dma = pltpu.SemaphoreType.DMA
    hbm = pl.BlockSpec(memory_space=pl.ANY)
    width = tensor_count * rows
    return pl.pallas_call(
        functools.partial(fused_kernel, tensor_count),
        out_shape=jax.ShapeDtypeStruct((stacks, serve, width), w.dtype),
        in_specs=[hbm] * 4,
        out_specs=hbm,
        scratch_shapes=[
            pltpu.VMEM((units, group, 2, UNIT, rows), w.dtype),
            pltpu.VMEM((units, tensor_count, UNIT, rows), w.dtype),
            pltpu.VMEM((relayed, group, 2, UNIT, rows), w.dtype),
            pltpu.VMEM((2, group, 2, rows, UNIT), w.dtype),
            pltpu.VMEM((tensor_count, stacks, rank, rows), w.dtype),
            pltpu.VMEM((stacks, rank, half), w.dtype),
            pltpu.VMEM((stacks, half), jnp.float32),
            pltpu.VMEM((UNIT, width), jnp.float32),
            pltpu.VMEM((2, UNIT, width), w.dtype),
            dma((2, group, 2)),
            dma((stacks, group, 2)),
            dma((units, tensor_count)),
            dma((relayed, group, 2)),
            dma((group, 2)),
            dma((tensor_count,)),
            dma,
            dma((tensor_count,)),
            dma((tensor_count,)),
            dma((tensor_count,)),
            dma((tensor_count,)),
            dma((2,)),
            dma((2, 2, 2)),
            dma((2,)),
            dma((2,)),
            dma((stacks,)),
        ],
        compiler_params=pltpu.CompilerParams(has_side_effects=True, vmem_limit_bytes=67_043_328),
    )(w, lt, r, m)


def fits(tensor_count, replica_count, stacks, rows, cols):
    if replica_count != 4 or tensor_count % 4 or cols % (tensor_count // 4):
        return False
    serve = cols // (tensor_count // 4)
    pieces = 7 * stacks * rows * cols // 6 + stacks * (serve // 2) * tensor_count * rows
    return rows % 128 == 0 and serve % (2 * UNIT) == 0 and pieces <= 30_000_000


def shards(base_weight, adapter_left, adapter_right, magnitude):
    tensor_count = lax.axis_size("tensor")
    replica_count = lax.axis_size("dp")
    experts, projections, rows, cols = base_weight.shape
    rank = adapter_left.shape[3]
    stacks = experts * projections
    group = tensor_count // replica_count
    serve = cols // group
    chunks = stacks if tensor_count <= 16 else 1
    relayed = (2 * (serve // 16) + 1) // 3 * 16

    if fits(tensor_count, replica_count, stacks, rows, cols):
        out = fused(
            base_weight.reshape(stacks, rows, cols),
            adapter_left.swapaxes(2, 3).reshape(stacks, rank, rows),
            adapter_right.reshape(stacks, rank, cols),
            magnitude.reshape(stacks, cols).astype(jnp.float32),
            tensor_count,
        )
        return out.reshape(experts, projections, serve, -1)
    s = flip(base_weight.reshape(stacks, rows, cols))
    if chunks == 1:
        s = s.reshape(1, stacks, group, serve, rows).swapaxes(1, 2)
    else:
        s = s.reshape(chunks, group, 1, serve, rows)
    g = exchange(s, tensor_count, replica_count, relayed).reshape(tensor_count, stacks, serve, rows)

    left = lax.all_gather(adapter_left.swapaxes(2, 3), "tensor", axis=3, tiled=True)
    right_all = lax.all_gather(adapter_right, "dp", axis=3, tiled=True)
    magnitude_all = lax.all_gather(magnitude, "dp", axis=2, tiled=True)
    start = lax.axis_index("tensor") * serve
    right = lax.dynamic_slice_in_dim(right_all, start, serve, 3).swapaxes(2, 3)
    strength = lax.dynamic_slice_in_dim(magnitude_all, start, serve, 2)
    out = merge(
        g,
        left.reshape(stacks, rank, -1),
        right.reshape(stacks, serve, rank),
        strength.reshape(stacks, serve, 1),
    )
    return out.reshape(experts, projections, serve, -1)


def solution(mesh):
    in_specs = (
        P(None, None, "tensor", "dp"),
        P(None, None, "tensor", None),
        P(None, None, None, "dp"),
        P(None, None, "dp"),
    )
    out_specs = P(None, None, "tensor", None)
    return jax.shard_map(shards, mesh=mesh, in_specs=in_specs, out_specs=out_specs, check_vma=False)
```

```python
import functools

import jax
import jax.numpy as jnp
from jax import lax
from jax.experimental import pallas as pl
from jax.experimental.pallas import tpu as pltpu
from jax.sharding import PartitionSpec as P

MESH = pl.DeviceIdType.MESH


def exchange_kernel(sizes, chunks, relayed, s, g, rb, recv, xs, cs, a_send, a_recv, b_send, r_send):
    tensor_count, replica_count = sizes
    group = tensor_count // replica_count
    half_t, half_r = tensor_count // 2, replica_count // 2
    serve = s.shape[3]
    parts = ((0, relayed), (relayed, serve - relayed))
    t, d = lax.axis_index("tensor"), lax.axis_index("dp")
    twin = lax.rem(d + half_r, replica_count)
    mate = d + 1 - 2 * lax.rem(d, 2)
    near = t // half_t == d // half_r
    far = jnp.logical_not(near)
    home = t // group
    is_home, is_twin = home == d, home == twin
    base = (t // half_t) * half_t
    other = half_t - base

    def near_source(i):
        return base + lax.rem(t - base + i, half_t)

    def far_source(i):
        return other + lax.rem(t - base + i, half_t)

    def own(k, j, p):
        return s.at[k, j, :, pl.ds(*parts[p])]

    def slot(ts, k, p):
        return g.at[ts, k, :, pl.ds(*parts[p])]

    def send(src, ts, k, p, sem, tensor, dp):
        return pltpu.make_async_remote_copy(
            src_ref=src, dst_ref=slot(ts, k, p), send_sem=sem, recv_sem=recv.at[ts, k, p],
            device_id={"tensor": tensor, "dp": dp}, device_id_type=MESH,
        )

    def to_twin(src, ts, k, p):
        return send(src, ts, k, p, xs.at[ts, k, p], t, twin)

    def to_mate(src, ts, k, p):
        return send(src, ts, k, p, cs.at[ts, k, p], t, mate)

    def to_relay(k, j):
        return pltpu.make_async_remote_copy(
            src_ref=own(k, j, 0), dst_ref=rb.at[k, j], send_sem=a_send.at[k, j], recv_sem=a_recv.at[k, j],
            device_id={"tensor": t, "dp": twin}, device_id_type=MESH,
        )

    def relay(k, j):
        return send(rb.at[k, j], t, k, 0, r_send.at[k, j], twin * group + j, d)

    def direct(k, j, p):
        return send(own(k, j, p), t, k, p, b_send.at[k, j, p], d * group + j, d)

    def keep(k, p):
        return pltpu.make_async_copy(own(k, lax.rem(t, group), p), slot(t, k, p), recv.at[t, k, p])

    def got(ts, k, p):
        to_mate(slot(ts, k, p), ts, k, p).wait_recv()

    def loop(count, body, first=0):
        lax.fori_loop(first, count, lambda i, c: (body(i), c)[1], 0)

    def each_piece(body):
        loop(chunks, lambda k: loop(group, lambda j: body(k, j)))

    def start_piece(k, j):
        leaves = d * group + j != t

        @pl.when(far)
        def _():
            to_relay(k, j).start()
            direct(k, j, 1).start()

        @pl.when(jnp.logical_and(near, leaves))
        def _():
            direct(k, j, 0).start()
            direct(k, j, 1).start()

        @pl.when(jnp.logical_not(leaves))
        def _():
            for p in range(2):
                src = own(k, j, p)
                to_twin(src, t, k, p).start()
                to_mate(src, t, k, p).start()
                keep(k, p).start()

    each_piece(start_piece)

    def pass_on(ts, k, p):
        got(ts, k, p)
        to_twin(slot(ts, k, p), ts, k, p).start()
        to_mate(slot(ts, k, p), ts, k, p).start()

    def hand_over(ts, k, p):
        got(ts, k, p)
        to_mate(slot(ts, k, p), ts, k, p).start()

    def relay_step(k):
        @pl.when(near)
        def _():
            def one(j):
                to_relay(k, j).wait_recv()
                relay(k, j).start()

            loop(group, one)

    def arrivals(k):
        @pl.when(is_home)
        def _():
            def one(i):
                pass_on(near_source(i), k, 0)
                pass_on(near_source(i), k, 1)

            loop(half_t, one, 1)
            loop(half_t, lambda i: pass_on(far_source(i), k, 1))

        @pl.when(is_twin)
        def _():
            loop(half_t, lambda i: pass_on(far_source(i), k, 0))

    def second_hand(k):
        @pl.when(is_home)
        def _():
            loop(half_t, lambda i: hand_over(far_source(i), k, 0))

        @pl.when(is_twin)
        def _():
            def one(i):
                hand_over(near_source(i), k, 0)
                hand_over(near_source(i), k, 1)

            loop(half_t, one)
            loop(half_t, lambda i: hand_over(far_source(i), k, 1))

    relay_step(0)

    def step(k):
        @pl.when(k + 1 < chunks)
        def _():
            relay_step(k + 1)

        arrivals(k)

        @pl.when(k > 0)
        def _():
            second_hand(k - 1)

    loop(chunks, step)
    second_hand(chunks - 1)

    serving = jnp.logical_or(is_home, is_twin)

    @pl.when(jnp.logical_not(serving))
    def _():
        def one(k, ts):
            got(ts, k, 0)
            got(ts, k, 1)

        loop(chunks, lambda k: loop(tensor_count, lambda ts: one(k, ts)))

    @pl.when(is_home)
    def _():
        def one(k):
            keep(k, 0).wait()
            keep(k, 1).wait()

        loop(chunks, one)

    def finish_piece(k, j):
        leaves = d * group + j != t

        @pl.when(far)
        def _():
            to_relay(k, j).wait_send()
            direct(k, j, 1).wait_send()

        @pl.when(near)
        def _():
            relay(k, j).wait_send()

        @pl.when(jnp.logical_and(near, leaves))
        def _():
            direct(k, j, 0).wait_send()
            direct(k, j, 1).wait_send()

    each_piece(finish_piece)

    @pl.when(serving)
    def _():
        def one(k, ts):
            to_mate(slot(ts, k, 0), ts, k, 0).wait_send()
            to_mate(slot(ts, k, 1), ts, k, 1).wait_send()

        loop(chunks, lambda k: loop(tensor_count, lambda ts: one(k, ts)))

    @pl.when(is_home)
    def _():
        def one(k, i):
            to_twin(slot(near_source(i), k, 0), near_source(i), k, 0).wait_send()
            to_twin(slot(near_source(i), k, 1), near_source(i), k, 1).wait_send()
            to_twin(slot(far_source(i), k, 1), far_source(i), k, 1).wait_send()

        loop(chunks, lambda k: loop(half_t, lambda i: one(k, i)))

    @pl.when(is_twin)
    def _():
        def one(k, i):
            to_twin(slot(far_source(i), k, 0), far_source(i), k, 0).wait_send()

        loop(chunks, lambda k: loop(half_t, lambda i: one(k, i)))


def exchange(s, tensor_count, replica_count, relayed):
    chunks, group, each, serve, rows = s.shape
    dma = pltpu.SemaphoreType.DMA
    g, _ = pl.pallas_call(
        functools.partial(exchange_kernel, (tensor_count, replica_count), chunks, relayed),
        out_shape=(
            jax.ShapeDtypeStruct((tensor_count, chunks, each, serve, rows), s.dtype),
            jax.ShapeDtypeStruct((chunks, group, each, relayed, rows), s.dtype),
        ),
        in_specs=[pl.BlockSpec(memory_space=pl.ANY)],
        out_specs=[pl.BlockSpec(memory_space=pl.ANY)] * 2,
        scratch_shapes=[dma((tensor_count, chunks, 2))] * 3
        + [dma((chunks, group))] * 2
        + [dma((chunks, group, 2)), dma((chunks, group))],
        compiler_params=pltpu.CompilerParams(has_side_effects=True),
    )(s)
    return g


def flip_kernel(w, o):
    o[0] = w[0].T


def flip(w):
    stacks, rows, cols = w.shape
    if rows % 128:
        return w.swapaxes(1, 2)
    wide = next(n for n in (512, 256, 128, cols) if cols % n == 0)
    return pl.pallas_call(
        flip_kernel,
        grid=(stacks, cols // wide),
        in_specs=[pl.BlockSpec((1, rows, wide), lambda e, c: (e, 0, c))],
        out_specs=pl.BlockSpec((1, wide, rows), lambda e, c: (e, c, 0)),
        out_shape=jax.ShapeDtypeStruct((stacks, cols, rows), w.dtype),
    )(w)


def merge_kernel(count, rows, g, left, right, magnitude, o, merged):
    squares = None
    for n in range(count):
        at = slice(n * rows, (n + 1) * rows)
        piece = g[n, 0].astype(jnp.float32) + jnp.dot(
            right[0], left[0, :, at], preferred_element_type=jnp.float32
        )
        merged[:, at] = piece
        total = jnp.sum(piece * piece, axis=1, keepdims=True)
        squares = total if squares is None else squares + total
    scaling = magnitude[0].astype(jnp.float32) / jnp.sqrt(squares + 1e-06)
    for n in range(count):
        at = slice(n * rows, (n + 1) * rows)
        o[0, :, at] = (merged[:, at] * scaling).astype(o.dtype)


def merge(g, left, right, magnitude):
    count, stacks, serve, rows = g.shape
    rank = right.shape[2]
    if rows % 128:
        joined = g.transpose(1, 2, 0, 3).reshape(stacks, serve, count * rows)
        merged = joined.astype(jnp.float32) + jnp.einsum(
            "xfr,xri->xfi", right, left, preferred_element_type=jnp.float32
        )
        squares = jnp.sum(merged * merged, axis=2, keepdims=True)
        scaling = magnitude.astype(jnp.float32) / jnp.sqrt(squares + 1e-06)
        return (merged * scaling).astype(g.dtype)
    tall = next(n for n in (256, 128, 64, 32, 16, serve) if serve % n == 0)
    return pl.pallas_call(
        functools.partial(merge_kernel, count, rows),
        grid=(stacks, serve // tall),
        in_specs=[
            pl.BlockSpec((count, 1, tall, rows), lambda e, f: (0, e, f, 0)),
            pl.BlockSpec((1, rank, count * rows), lambda e, f: (e, 0, 0)),
            pl.BlockSpec((1, tall, rank), lambda e, f: (e, f, 0)),
            pl.BlockSpec((1, tall, 1), lambda e, f: (e, f, 0)),
        ],
        out_specs=pl.BlockSpec((1, tall, count * rows), lambda e, f: (e, f, 0)),
        out_shape=jax.ShapeDtypeStruct((stacks, serve, count * rows), g.dtype),
        scratch_shapes=[pltpu.VMEM((tall, count * rows), jnp.float32)],
    )(g, left, right, magnitude)


UNIT = 128
RELAY_LAG, FORWARD_LAG, MERGE_LAG = 1, 2, 2
CREDIT_LAG, KEPT = 3, 8


def fused_kernel(
    tensor_count, lead, w, lt, r, m, first, middle, s, g, rb, win, left, right, strength, merged,
    w_sem, s_send, s_twin, g_recv, rb_recv, rb_send, f_send, l_own, l_recv, l_send, l_mate, l_twin,
    p_recv, p_send, o_send, o_recv, credit,
):
    units, _, unit, rows = g.shape
    half_t = tensor_count // 2
    group = half_t // 2
    stacks, half = strength.shape
    serve = 2 * half
    per = half // unit
    t, d = lax.axis_index("tensor"), lax.axis_index("dp")
    x, c = d // 2, lax.rem(d, 2)
    twin = lax.rem(d + 2, 4)
    mate = d + 1 - 2 * c
    near = t // half_t == x
    far = jnp.logical_not(near)
    home = t // group == d
    base = (t // half_t) * half_t
    other = half_t - base

    def near_source(i):
        return base + lax.rem(t - base + i, half_t)

    def far_source(i):
        return other + lax.rem(t - base + i, half_t)

    def loop(count, body, first=0):
        lax.fori_loop(first, count, lambda i, carry: (body(i), carry)[1], 0)

    def is_direct(v, h):
        return lax.rem(v + h, 3) == 1

    def direct_before(v, h):
        return (v + 1 + h) // 3

    def relay_index(v, h):
        return v - direct_before(v, h)

    def remote(src, dst, send_sem, recv_sem, tensor, dp):
        return pltpu.make_async_remote_copy(
            src_ref=src, dst_ref=dst, send_sem=send_sem, recv_sem=recv_sem,
            device_id={"tensor": tensor, "dp": dp}, device_id_type=MESH,
        )

    pairs = [(j, h) for j in range(group) for h in range(2)]

    def load(v, j, h):
        k, q = v // per, lax.rem(v, per)
        at = pl.multiple_of(j * serve + h * half + q * unit, unit)
        slot = lax.rem(v, 2)
        return pltpu.make_async_copy(
            w.at[k, :, pl.ds(at, unit)], win.at[slot, j, h], w_sem.at[slot, j, h]
        )

    def start_load(v):
        for j, h in pairs:
            load(v, j, h).start()

    def piece(v, j, h):
        return s.at[v // 2, lax.rem(v, 2) * half_t + j * 2 + h]

    def to_server(v, j, h):
        return remote(
            piece(v, j, h), g.at[v, t], s_send.at[v // 2, j, h], g_recv.at[v, t],
            d * group + j, x * 2 + h,
        )

    level = jnp.logical_and(near, d == t // group)

    def to_twin_server(v, j, h):
        return remote(
            piece(v, j, h), g.at[v, t], s_twin.at[v // 2, j, h], g_recv.at[v, t],
            d * group + j, (1 - x) * 2 + h,
        )

    def to_relay(v, j, h):
        at = relay_index(v, h)
        return remote(
            piece(v, j, h), rb.at[at, j, h], s_send.at[v // 2, j, h], rb_recv.at[at, j, h], t, twin
        )

    def stays(j, h):
        return jnp.logical_and(d * group + j == t, c == h)

    def flip_and_send(v):
        slot = lax.rem(v, 2)
        for j, h in pairs:
            load(v, j, h).wait()
            turned = win[slot, j, h].T
            s[v // 2, lax.rem(v, 2) * half_t + j * 2 + h] = turned
            own = stays(j, h)

            @pl.when(own)
            def _():
                g[v, t] = turned

            by_hand = jnp.logical_and(far, jnp.logical_not(is_direct(v, h)))

            @pl.when(by_hand)
            def _():
                to_relay(v, j, h).start()

            @pl.when(jnp.logical_not(jnp.logical_or(own, by_hand)))
            def _():
                to_server(v, j, h).start()

            @pl.when(level)
            def _():
                to_twin_server(v, j, h).start()

        @pl.when(v + 2 < units)
        def _():
            start_load(v + 2)

    def relay(v, j, h):
        return remote(
            rb.at[relay_index(v, h), j, h], g.at[v, t], rb_send.at[j, h], g_recv.at[v, t],
            twin * group + j, x * 2 + h,
        )

    def relay_step(v):
        for j, h in pairs:

            @pl.when(jnp.logical_and(near, jnp.logical_not(is_direct(v, h))))
            def _():
                to_relay(v, j, h).wait_recv()
                relay(v, j, h).start()

    def forward(v, ts):
        return remote(g.at[v, ts], g.at[v, ts], f_send.at[v, ts], g_recv.at[v, ts], t, twin)

    def got(v, ts):
        forward(v, ts).wait_recv()

    def pass_on(v, ts):
        got(v, ts)
        forward(v, ts).start()

    def arrivals(v):
        @pl.when(near)
        def _():
            @pl.when(jnp.logical_not(home))
            def _():
                got(v, t)

            def take_near(i):
                ts = near_source(i)
                got(v, ts)

                @pl.when(ts // group != t // group)
                def _():
                    forward(v, ts).start()

            loop(half_t, take_near, 1)

            @pl.when(is_direct(v, c))
            def _():
                loop(half_t, lambda i: pass_on(v, far_source(i)))

        @pl.when(jnp.logical_and(far, jnp.logical_not(is_direct(v, c))))
        def _():
            loop(half_t, lambda i: pass_on(v, far_source(i)))

    def second_hand(v):
        @pl.when(far)
        def _():
            loop(half_t, lambda i: got(v, near_source(i)))

            @pl.when(is_direct(v, c))
            def _():
                loop(half_t, lambda i: got(v, far_source(i)))

        @pl.when(jnp.logical_and(near, jnp.logical_not(is_direct(v, c))))
        def _():
            loop(half_t, lambda i: got(v, far_source(i)))

    def forwarded(v):
        def near_sent(i):
            @pl.when(near_source(i) // group != t // group)
            def _():
                forward(v, near_source(i)).wait_send()

        @pl.when(near)
        def _():
            loop(half_t, near_sent)

        @pl.when(near == is_direct(v, c))
        def _():
            loop(half_t, lambda i: forward(v, far_source(i)).wait_send())

    def to_mate(v, place):
        return remote(g.at[v], place, o_send.at[v], o_recv.at[v], t, mate)

    spare = units // 2

    def hand_to_mate(v):
        @pl.when(v < lead)
        def _():
            to_mate(v, first.at[v]).start()

        @pl.when(jnp.logical_and(v >= lead, v < spare))
        def _():
            to_mate(v, middle.at[v - lead]).start()

        @pl.when(v >= spare)
        def _():
            pl.semaphore_wait(credit, 1)
            to_mate(v, s.at[v - spare]).start()

    def give_credit(v):
        at = v - spare
        both = s.at[at, 0:2]
        for j, h in pairs:

            @pl.when(jnp.logical_not(stays(j, h)))
            def _():
                remote(both, both, s_send.at[at, j, h], o_recv.at[0], t, mate).wait_send()

            @pl.when(level)
            def _():
                remote(both, both, s_twin.at[at, j, h], o_recv.at[0], t, mate).wait_send()

        pl.semaphore_signal(
            credit, inc=1, device_id={"tensor": t, "dp": mate}, device_id_type=MESH
        )

    def merge_unit(v):
        k, q = v // per, lax.rem(v, per)
        lanes = pl.ds(pl.multiple_of(q * unit, unit), unit)
        second_hand(v)
        factor = right[k, :, lanes]
        squares = jnp.zeros((unit, 128), jnp.float32)
        for n in range(tensor_count):
            piece = g[v, n].astype(jnp.float32) + lax.dot_general(
                factor, left[n, k], (((0,), (0,)), ((), ())), preferred_element_type=jnp.float32
            )
            merged[:, n * rows : (n + 1) * rows] = piece
            for b in range(rows // 128):
                part = piece[:, b * 128 : (b + 1) * 128]
                squares = squares + part * part
        total = jnp.sum(squares, axis=1, keepdims=True)
        stack = lax.broadcasted_iota(jnp.int32, (stacks, unit), 0)
        chosen = jnp.sum(jnp.where(stack == k, strength[:, lanes], 0.0), axis=0, keepdims=True)
        wide = jnp.broadcast_to(chosen, (unit, unit)).T
        scaling = wide / jnp.sqrt(total + 1e-06)

        forwarded(v)
        for n in range(tensor_count):
            for b in range(rows // 128):
                at = slice(b * 128, (b + 1) * 128)
                wide_at = slice(n * rows + b * 128, n * rows + (b + 1) * 128)
                g[v, n, :, at] = (merged[:, wide_at] * scaling).astype(g.dtype)
        hand_to_mate(v)

    carrier = lax.rem(t, 2) == c

    def left_out(ts):
        return remote(lt, left.at[t], l_send.at[ts], l_recv.at[t], ts, d)

    def left_mate(ts):
        return remote(left.at[ts], left.at[ts], l_mate.at[ts], l_recv.at[ts], t, mate)

    def left_twin(ts):
        return remote(left.at[ts], left.at[ts], l_twin.at[ts], l_recv.at[ts], t, twin)

    own_left = pltpu.make_async_copy(lt, left.at[t], l_own)

    def factors(h, dp):
        at = pl.multiple_of(lax.rem(t, group) * serve + h * half, unit)
        way = dp // 2
        return (
            remote(r.at[:, :, pl.ds(at, half)], right, p_send.at[0, way, h], p_recv.at[0], t, dp),
            remote(m.at[:, pl.ds(at, half)], strength, p_send.at[1, way, h], p_recv.at[1], t, dp),
        )

    def own_factors(h):
        at = pl.multiple_of(lax.rem(t, group) * serve + h * half, unit)
        return (
            pltpu.make_async_copy(r.at[:, :, pl.ds(at, half)], right, p_recv.at[0]),
            pltpu.make_async_copy(m.at[:, pl.ds(at, half)], strength, p_recv.at[1]),
        )

    def each_factor(remote_do, own_do):
        for way in range(2):
            for h in range(2):
                dp = way * 2 + h

                if remote_do:

                    @pl.when(jnp.logical_and(home, d != dp))
                    def _():
                        for copy in factors(h, dp):
                            remote_do(copy)

                if own_do:

                    @pl.when(jnp.logical_and(home, d == dp))
                    def _():
                        for copy in own_factors(h):
                            own_do(copy)

    start_load(0)
    start_load(1)
    own_left.start()

    @pl.when(carrier)
    def _():
        loop(half_t, lambda i: left_out(near_source(i)).start(), 1)

        @pl.when(far)
        def _():
            loop(half_t, lambda i: left_out(far_source(i)).start())

    each_factor(lambda copy: copy.start(), lambda copy: copy.start())

    def carries(ts):
        return lax.rem(ts, 2) == c

    def spread(ts, across):
        @pl.when(carries(ts))
        def _():
            left_mate(ts).wait_recv()
            left_mate(ts).start()
            if across:
                left_twin(ts).start()

    def take(ts):
        @pl.when(jnp.logical_not(carries(ts)))
        def _():
            left_mate(ts).wait_recv()

    def spread_first():
        loop(half_t, lambda i: spread(near_source(i), False), 1)

        @pl.when(near)
        def _():
            loop(half_t, lambda i: spread(far_source(i), True))

    def spread_second():
        @pl.when(far)
        def _():
            loop(half_t, lambda i: spread(far_source(i), False))

    def take_factors():
        own_left.wait()
        loop(half_t, lambda i: take(near_source(i)), 1)
        loop(half_t, lambda i: take(far_source(i)))

        @pl.when(jnp.logical_not(home))
        def _():
            for copy in factors(0, mate):
                copy.wait_recv()

        each_factor(None, lambda copy: copy.wait())

    def step(u):
        @pl.when(u < units)
        def _():
            flip_and_send(u)

        v = u - RELAY_LAG

        @pl.when(jnp.logical_and(v >= 0, v < units))
        def _():
            relay_step(v)

        v = u - FORWARD_LAG

        @pl.when(jnp.logical_and(v >= 0, v < units))
        def _():
            arrivals(v)

        v = u - CREDIT_LAG

        @pl.when(jnp.logical_and(v >= spare, v < units))
        def _():
            give_credit(v)

        for at, what in enumerate((spread_first, spread_second, take_factors)):
            pl.when(u == FORWARD_LAG + at)(what)

        v = u - FORWARD_LAG - MERGE_LAG

        @pl.when(v >= 0)
        def _():
            merge_unit(v)

    loop(units + FORWARD_LAG + MERGE_LAG, step)

    def last(v):
        to_mate(v, g.at[v]).wait_send()
        to_mate(v, g.at[v]).wait_recv()

    loop(units, last)

    @pl.when(near)
    def _():
        for j, h in pairs:
            sent = rb.at[0 : units - (units + 1 + h) // 3, j, h]
            remote(sent, sent, rb_send.at[j, h], g_recv.at[0, 0], t, twin).wait_send()

    @pl.when(carrier)
    def _():
        loop(half_t, lambda i: left_out(near_source(i)).wait_send(), 1)

        @pl.when(far)
        def _():
            loop(half_t, lambda i: left_out(far_source(i)).wait_send())

    def left_sent(ts, across):
        @pl.when(lax.rem(ts, 2) == c)
        def _():
            left_mate(ts).wait_send()
            if across:

                @pl.when(near)
                def _():
                    left_twin(ts).wait_send()

    loop(half_t, lambda i: left_sent(near_source(i), False), 1)
    loop(half_t, lambda i: left_sent(far_source(i), True))
    each_factor(lambda copy: copy.wait_send(), None)


def place_kernel(stacks, first, middle, last, own, o, held, stage, in_sem, out_sem):
    c = lax.rem(lax.axis_index("dp"), 2)
    units, count, unit, rows = own.shape
    half = o.shape[1] // 2
    per = units // stacks
    lead, kept = first.shape[0], middle.shape[0]
    depth = stage.shape[0]

    def fetch(v):
        slot = lax.rem(v, 2)
        return pltpu.make_async_copy(first.at[v], held.at[slot], in_sem.at[slot])

    def leave(slot, k, at):
        return pltpu.make_async_copy(stage.at[slot], o.at[k, at], out_sem.at[slot])

    def place(src, v, core, turn):
        k, q = v // per, lax.rem(v, per)
        at = pl.ds(pl.multiple_of(core * half + q * unit, unit), unit)
        slot = lax.rem(turn, depth)

        @pl.when(turn >= depth)
        def _():
            leave(slot, k, at).wait()

        for n in range(count):
            stage[slot, :, n * rows : (n + 1) * rows] = src[n]
        leave(slot, k, at).start()

    def loop(begin, end, body):
        lax.fori_loop(begin, end, lambda v, carry: (body(v), carry)[1], 0)

    def from_hbm(v):
        fetch(v).wait()
        place(held.at[lax.rem(v, 2)], v, 1 - c, units + v)

        @pl.when(v + 2 < lead)
        def _():
            fetch(v + 2).start()

    for v in range(min(2, lead)):
        fetch(v).start()
    loop(0, units, lambda v: place(own.at[v], v, c, v))
    loop(0, lead, from_hbm)
    loop(lead, lead + kept, lambda v: place(middle.at[v - lead], v, 1 - c, units + v))
    loop(lead + kept, units, lambda v: place(last.at[v - lead - kept], v, 1 - c, units + v))
    for slot in range(depth):
        leave(slot, 0, pl.ds(0, unit)).wait()


def fused(w, lt, r, m, tensor_count):
    stacks, rows, cols = w.shape
    rank = lt.shape[1]
    group = tensor_count // 4
    serve = cols // group
    half = serve // 2
    per = half // UNIT
    units = stacks * per
    relayed = units - (units + 1) // 3
    dma = pltpu.SemaphoreType.DMA
    hbm = pl.BlockSpec(memory_space=pl.ANY)
    width = tensor_count * rows
    vmem = pl.BlockSpec(memory_space=pltpu.VMEM)
    spare = units // 2
    lead = max(1, spare - KEPT)
    block = (tensor_count, UNIT, rows)
    parts = pl.pallas_call(
        functools.partial(fused_kernel, tensor_count, lead),
        out_shape=(
            jax.ShapeDtypeStruct((lead, *block), w.dtype),
            pltpu.VMEM((spare - lead, *block), w.dtype),
            pltpu.VMEM((spare, *block), w.dtype),
            pltpu.VMEM((units, *block), w.dtype),
        ),
        in_specs=[hbm] * 4,
        out_specs=(hbm, vmem, vmem, vmem),
        scratch_shapes=[
            pltpu.VMEM((relayed, group, 2, UNIT, rows), w.dtype),
            pltpu.VMEM((2, group, 2, rows, UNIT), w.dtype),
            pltpu.VMEM((tensor_count, stacks, rank, rows), w.dtype),
            pltpu.VMEM((stacks, rank, half), w.dtype),
            pltpu.VMEM((stacks, half), jnp.float32),
            pltpu.VMEM((UNIT, width), jnp.float32),
            dma((2, group, 2)),
            dma((spare, group, 2)),
            dma((spare, group, 2)),
            dma((units, tensor_count)),
            dma((relayed, group, 2)),
            dma((group, 2)),
            dma((units, tensor_count)),
            dma,
            dma((tensor_count,)),
            dma((tensor_count,)),
            dma((tensor_count,)),
            dma((tensor_count,)),
            dma((2,)),
            dma((2, 2, 2)),
            dma((units,)),
            dma((units,)),
            pltpu.SemaphoreType.REGULAR,
        ],
        compiler_params=pltpu.CompilerParams(has_side_effects=True, vmem_limit_bytes=14200000),
    )(w, lt, r, m)
    return pl.pallas_call(
        functools.partial(place_kernel, stacks),
        out_shape=jax.ShapeDtypeStruct((stacks, serve, width), w.dtype),
        in_specs=[hbm, vmem, vmem, vmem],
        out_specs=hbm,
        scratch_shapes=[
            pltpu.VMEM((2, *block), w.dtype),
            pltpu.VMEM((4, UNIT, width), w.dtype),
            dma((2,)),
            dma((4,)),
        ],
        compiler_params=pltpu.CompilerParams(vmem_limit_bytes=8_000_000),
    )(parts[0], *(pltpu.with_memory_space_constraint(p, pltpu.VMEM) for p in parts[1:]))


def fits(tensor_count, replica_count, stacks, rows, cols):
    if replica_count != 4 or tensor_count % 8 or cols % (tensor_count // 2 * UNIT) or rows % 128:
        return False
    units = stacks * (cols // (tensor_count // 2 * UNIT))
    pieces = units * tensor_count * UNIT * rows
    return units % 2 == 0 and units // 2 > KEPT and pieces <= 15_000_000


def shards(base_weight, adapter_left, adapter_right, magnitude):
    tensor_count = lax.axis_size("tensor")
    replica_count = lax.axis_size("dp")
    experts, projections, rows, cols = base_weight.shape
    rank = adapter_left.shape[3]
    stacks = experts * projections
    group = tensor_count // replica_count
    serve = cols // group
    chunks = stacks if tensor_count <= 16 else 1
    relayed = (2 * (serve // 16) + 1) // 3 * 16

    if fits(tensor_count, replica_count, stacks, rows, cols):
        out = fused(
            base_weight.reshape(stacks, rows, cols),
            adapter_left.swapaxes(2, 3).reshape(stacks, rank, rows),
            adapter_right.reshape(stacks, rank, cols),
            magnitude.reshape(stacks, cols).astype(jnp.float32),
            tensor_count,
        )
        return out.reshape(experts, projections, serve, -1)
    s = flip(base_weight.reshape(stacks, rows, cols))
    if chunks == 1:
        s = s.reshape(1, stacks, group, serve, rows).swapaxes(1, 2)
    else:
        s = s.reshape(chunks, group, 1, serve, rows)
    g = exchange(s, tensor_count, replica_count, relayed).reshape(tensor_count, stacks, serve, rows)

    left = lax.all_gather(adapter_left.swapaxes(2, 3), "tensor", axis=3, tiled=True)
    right_all = lax.all_gather(adapter_right, "dp", axis=3, tiled=True)
    magnitude_all = lax.all_gather(magnitude, "dp", axis=2, tiled=True)
    start = lax.axis_index("tensor") * serve
    right = lax.dynamic_slice_in_dim(right_all, start, serve, 3).swapaxes(2, 3)
    strength = lax.dynamic_slice_in_dim(magnitude_all, start, serve, 2)
    out = merge(
        g,
        left.reshape(stacks, rank, -1),
        right.reshape(stacks, serve, rank),
        strength.reshape(stacks, serve, 1),
    )
    return out.reshape(experts, projections, serve, -1)


def solution(mesh):
    in_specs = (
        P(None, None, "tensor", "dp"),
        P(None, None, "tensor", None),
        P(None, None, None, "dp"),
        P(None, None, "dp"),
    )
    out_specs = P(None, None, "tensor", None)
    return jax.shard_map(shards, mesh=mesh, in_specs=in_specs, out_specs=out_specs, check_vma=False)
```

```python
import functools

import jax
import jax.numpy as jnp
from jax import lax
from jax.experimental import pallas as pl
from jax.experimental.pallas import tpu as pltpu
from jax.sharding import PartitionSpec as P

MESH = pl.DeviceIdType.MESH


def exchange_kernel(sizes, chunks, relayed, s, g, rb, recv, xs, cs, a_send, a_recv, b_send, r_send):
    tensor_count, replica_count = sizes
    group = tensor_count // replica_count
    half_t, half_r = tensor_count // 2, replica_count // 2
    serve = s.shape[3]
    parts = ((0, relayed), (relayed, serve - relayed))
    t, d = lax.axis_index("tensor"), lax.axis_index("dp")
    twin = lax.rem(d + half_r, replica_count)
    mate = d + 1 - 2 * lax.rem(d, 2)
    near = t // half_t == d // half_r
    far = jnp.logical_not(near)
    home = t // group
    is_home, is_twin = home == d, home == twin
    base = (t // half_t) * half_t
    other = half_t - base

    def near_source(i):
        return base + lax.rem(t - base + i, half_t)

    def far_source(i):
        return other + lax.rem(t - base + i, half_t)

    def own(k, j, p):
        return s.at[k, j, :, pl.ds(*parts[p])]

    def slot(ts, k, p):
        return g.at[ts, k, :, pl.ds(*parts[p])]

    def send(src, ts, k, p, sem, tensor, dp):
        return pltpu.make_async_remote_copy(
            src_ref=src, dst_ref=slot(ts, k, p), send_sem=sem, recv_sem=recv.at[ts, k, p],
            device_id={"tensor": tensor, "dp": dp}, device_id_type=MESH,
        )

    def to_twin(src, ts, k, p):
        return send(src, ts, k, p, xs.at[ts, k, p], t, twin)

    def to_mate(src, ts, k, p):
        return send(src, ts, k, p, cs.at[ts, k, p], t, mate)

    def to_relay(k, j):
        return pltpu.make_async_remote_copy(
            src_ref=own(k, j, 0), dst_ref=rb.at[k, j], send_sem=a_send.at[k, j], recv_sem=a_recv.at[k, j],
            device_id={"tensor": t, "dp": twin}, device_id_type=MESH,
        )

    def relay(k, j):
        return send(rb.at[k, j], t, k, 0, r_send.at[k, j], twin * group + j, d)

    def direct(k, j, p):
        return send(own(k, j, p), t, k, p, b_send.at[k, j, p], d * group + j, d)

    def keep(k, p):
        return pltpu.make_async_copy(own(k, lax.rem(t, group), p), slot(t, k, p), recv.at[t, k, p])

    def got(ts, k, p):
        to_mate(slot(ts, k, p), ts, k, p).wait_recv()

    def loop(count, body, first=0):
        lax.fori_loop(first, count, lambda i, c: (body(i), c)[1], 0)

    def each_piece(body):
        loop(chunks, lambda k: loop(group, lambda j: body(k, j)))

    def start_piece(k, j):
        leaves = d * group + j != t

        @pl.when(far)
        def _():
            to_relay(k, j).start()
            direct(k, j, 1).start()

        @pl.when(jnp.logical_and(near, leaves))
        def _():
            direct(k, j, 0).start()
            direct(k, j, 1).start()

        @pl.when(jnp.logical_not(leaves))
        def _():
            for p in range(2):
                src = own(k, j, p)
                to_twin(src, t, k, p).start()
                to_mate(src, t, k, p).start()
                keep(k, p).start()

    each_piece(start_piece)

    def pass_on(ts, k, p):
        got(ts, k, p)
        to_twin(slot(ts, k, p), ts, k, p).start()
        to_mate(slot(ts, k, p), ts, k, p).start()

    def hand_over(ts, k, p):
        got(ts, k, p)
        to_mate(slot(ts, k, p), ts, k, p).start()

    def relay_step(k):
        @pl.when(near)
        def _():
            def one(j):
                to_relay(k, j).wait_recv()
                relay(k, j).start()

            loop(group, one)

    def arrivals(k):
        @pl.when(is_home)
        def _():
            def one(i):
                pass_on(near_source(i), k, 0)
                pass_on(near_source(i), k, 1)

            loop(half_t, one, 1)
            loop(half_t, lambda i: pass_on(far_source(i), k, 1))

        @pl.when(is_twin)
        def _():
            loop(half_t, lambda i: pass_on(far_source(i), k, 0))

    def second_hand(k):
        @pl.when(is_home)
        def _():
            loop(half_t, lambda i: hand_over(far_source(i), k, 0))

        @pl.when(is_twin)
        def _():
            def one(i):
                hand_over(near_source(i), k, 0)
                hand_over(near_source(i), k, 1)

            loop(half_t, one)
            loop(half_t, lambda i: hand_over(far_source(i), k, 1))

    relay_step(0)

    def step(k):
        @pl.when(k + 1 < chunks)
        def _():
            relay_step(k + 1)

        arrivals(k)

        @pl.when(k > 0)
        def _():
            second_hand(k - 1)

    loop(chunks, step)
    second_hand(chunks - 1)

    serving = jnp.logical_or(is_home, is_twin)

    @pl.when(jnp.logical_not(serving))
    def _():
        def one(k, ts):
            got(ts, k, 0)
            got(ts, k, 1)

        loop(chunks, lambda k: loop(tensor_count, lambda ts: one(k, ts)))

    @pl.when(is_home)
    def _():
        def one(k):
            keep(k, 0).wait()
            keep(k, 1).wait()

        loop(chunks, one)

    def finish_piece(k, j):
        leaves = d * group + j != t

        @pl.when(far)
        def _():
            to_relay(k, j).wait_send()
            direct(k, j, 1).wait_send()

        @pl.when(near)
        def _():
            relay(k, j).wait_send()

        @pl.when(jnp.logical_and(near, leaves))
        def _():
            direct(k, j, 0).wait_send()
            direct(k, j, 1).wait_send()

    each_piece(finish_piece)

    @pl.when(serving)
    def _():
        def one(k, ts):
            to_mate(slot(ts, k, 0), ts, k, 0).wait_send()
            to_mate(slot(ts, k, 1), ts, k, 1).wait_send()

        loop(chunks, lambda k: loop(tensor_count, lambda ts: one(k, ts)))

    @pl.when(is_home)
    def _():
        def one(k, i):
            to_twin(slot(near_source(i), k, 0), near_source(i), k, 0).wait_send()
            to_twin(slot(near_source(i), k, 1), near_source(i), k, 1).wait_send()
            to_twin(slot(far_source(i), k, 1), far_source(i), k, 1).wait_send()

        loop(chunks, lambda k: loop(half_t, lambda i: one(k, i)))

    @pl.when(is_twin)
    def _():
        def one(k, i):
            to_twin(slot(far_source(i), k, 0), far_source(i), k, 0).wait_send()

        loop(chunks, lambda k: loop(half_t, lambda i: one(k, i)))


def exchange(s, tensor_count, replica_count, relayed):
    chunks, group, each, serve, rows = s.shape
    dma = pltpu.SemaphoreType.DMA
    g, _ = pl.pallas_call(
        functools.partial(exchange_kernel, (tensor_count, replica_count), chunks, relayed),
        out_shape=(
            jax.ShapeDtypeStruct((tensor_count, chunks, each, serve, rows), s.dtype),
            jax.ShapeDtypeStruct((chunks, group, each, relayed, rows), s.dtype),
        ),
        in_specs=[pl.BlockSpec(memory_space=pl.ANY)],
        out_specs=[pl.BlockSpec(memory_space=pl.ANY)] * 2,
        scratch_shapes=[dma((tensor_count, chunks, 2))] * 3
        + [dma((chunks, group))] * 2
        + [dma((chunks, group, 2)), dma((chunks, group))],
        compiler_params=pltpu.CompilerParams(has_side_effects=True),
    )(s)
    return g


def flip_kernel(w, o):
    o[0] = w[0].T


def flip(w):
    stacks, rows, cols = w.shape
    if rows % 128:
        return w.swapaxes(1, 2)
    wide = next(n for n in (512, 256, 128, cols) if cols % n == 0)
    return pl.pallas_call(
        flip_kernel,
        grid=(stacks, cols // wide),
        in_specs=[pl.BlockSpec((1, rows, wide), lambda e, c: (e, 0, c))],
        out_specs=pl.BlockSpec((1, wide, rows), lambda e, c: (e, c, 0)),
        out_shape=jax.ShapeDtypeStruct((stacks, cols, rows), w.dtype),
    )(w)


def merge_kernel(count, rows, g, left, right, magnitude, o, merged):
    squares = None
    for n in range(count):
        at = slice(n * rows, (n + 1) * rows)
        piece = g[n, 0].astype(jnp.float32) + jnp.dot(
            right[0], left[0, :, at], preferred_element_type=jnp.float32
        )
        merged[:, at] = piece
        total = jnp.sum(piece * piece, axis=1, keepdims=True)
        squares = total if squares is None else squares + total
    scaling = magnitude[0].astype(jnp.float32) / jnp.sqrt(squares + 1e-06)
    for n in range(count):
        at = slice(n * rows, (n + 1) * rows)
        o[0, :, at] = (merged[:, at] * scaling).astype(o.dtype)


def merge(g, left, right, magnitude):
    count, stacks, serve, rows = g.shape
    rank = right.shape[2]
    if rows % 128:
        joined = g.transpose(1, 2, 0, 3).reshape(stacks, serve, count * rows)
        merged = joined.astype(jnp.float32) + jnp.einsum(
            "xfr,xri->xfi", right, left, preferred_element_type=jnp.float32
        )
        squares = jnp.sum(merged * merged, axis=2, keepdims=True)
        scaling = magnitude.astype(jnp.float32) / jnp.sqrt(squares + 1e-06)
        return (merged * scaling).astype(g.dtype)
    tall = next(n for n in (256, 128, 64, 32, 16, serve) if serve % n == 0)
    return pl.pallas_call(
        functools.partial(merge_kernel, count, rows),
        grid=(stacks, serve // tall),
        in_specs=[
            pl.BlockSpec((count, 1, tall, rows), lambda e, f: (0, e, f, 0)),
            pl.BlockSpec((1, rank, count * rows), lambda e, f: (e, 0, 0)),
            pl.BlockSpec((1, tall, rank), lambda e, f: (e, f, 0)),
            pl.BlockSpec((1, tall, 1), lambda e, f: (e, f, 0)),
        ],
        out_specs=pl.BlockSpec((1, tall, count * rows), lambda e, f: (e, f, 0)),
        out_shape=jax.ShapeDtypeStruct((stacks, serve, count * rows), g.dtype),
        scratch_shapes=[pltpu.VMEM((tall, count * rows), jnp.float32)],
    )(g, left, right, magnitude)


UNIT = 128
RELAY_LAG, FORWARD_LAG, MERGE_LAG = 1, 2, 2
CREDIT_LAG, KEPT, STAGED = 3, 8, 6


def fused_kernel(
    tensor_count, lead, w, lt, r, m, first, middle, s, g, rb, win, left, right, strength, merged,
    w_sem, s_send, s_twin, g_recv, rb_recv, rb_send, f_send, l_own, l_recv, l_send, l_mate, l_twin,
    p_recv, p_send, o_send, o_recv, credit,
):
    units, _, unit, rows = g.shape
    half_t = tensor_count // 2
    group = half_t // 2
    experts, projections, half = strength.shape
    serve = 2 * half
    per = half // unit
    t, d = lax.axis_index("tensor"), lax.axis_index("dp")
    x, c = d // 2, lax.rem(d, 2)
    twin = lax.rem(d + 2, 4)
    mate = d + 1 - 2 * c
    near = t // half_t == x
    far = jnp.logical_not(near)
    home = t // group == d
    base = (t // half_t) * half_t
    other = half_t - base

    def near_source(i):
        return base + lax.rem(t - base + i, half_t)

    def far_source(i):
        return other + lax.rem(t - base + i, half_t)

    def loop(count, body, first=0):
        lax.fori_loop(first, count, lambda i, carry: (body(i), carry)[1], 0)

    def is_direct(v, h):
        return lax.rem(v + h, 3) == 1

    def direct_before(v, h):
        return (v + 1 + h) // 3

    def relay_index(v, h):
        return v - direct_before(v, h)

    def remote(src, dst, send_sem, recv_sem, tensor, dp):
        return pltpu.make_async_remote_copy(
            src_ref=src, dst_ref=dst, send_sem=send_sem, recv_sem=recv_sem,
            device_id={"tensor": tensor, "dp": dp}, device_id_type=MESH,
        )

    pairs = [(j, h) for j in range(group) for h in range(2)]

    def load(v, j, h):
        k, q = v // per, lax.rem(v, per)
        at = pl.multiple_of(j * serve + h * half + q * unit, unit)
        slot = lax.rem(v, 2)
        return pltpu.make_async_copy(
            w.at[k, :, pl.ds(at, unit)], win.at[slot, j, h], w_sem.at[slot, j, h]
        )

    def start_load(v):
        for j, h in pairs:
            load(v, j, h).start()

    def piece(v, j, h):
        return s.at[v // 2, lax.rem(v, 2) * half_t + j * 2 + h]

    def to_server(v, j, h):
        return remote(
            piece(v, j, h), g.at[v, t], s_send.at[v // 2, j, h], g_recv.at[v, t],
            d * group + j, x * 2 + h,
        )

    level = jnp.logical_and(near, d == t // group)

    def to_twin_server(v, j, h):
        return remote(
            piece(v, j, h), g.at[v, t], s_twin.at[v // 2, j, h], g_recv.at[v, t],
            d * group + j, (1 - x) * 2 + h,
        )

    def to_relay(v, j, h):
        at = relay_index(v, h)
        return remote(
            piece(v, j, h), rb.at[at, j, h], s_send.at[v // 2, j, h], rb_recv.at[at, j, h], t, twin
        )

    def stays(j, h):
        return jnp.logical_and(d * group + j == t, c == h)

    def flip_and_send(v):
        slot = lax.rem(v, 2)
        for j, h in pairs:
            load(v, j, h).wait()
            turned = win[slot, j, h].T
            s[v // 2, lax.rem(v, 2) * half_t + j * 2 + h] = turned
            own = stays(j, h)

            @pl.when(own)
            def _():
                g[v, t] = turned

            by_hand = jnp.logical_and(far, jnp.logical_not(is_direct(v, h)))

            @pl.when(by_hand)
            def _():
                to_relay(v, j, h).start()

            @pl.when(jnp.logical_not(jnp.logical_or(own, by_hand)))
            def _():
                to_server(v, j, h).start()

            @pl.when(level)
            def _():
                to_twin_server(v, j, h).start()

        @pl.when(v + 2 < units)
        def _():
            start_load(v + 2)

    def relay(v, j, h):
        return remote(
            rb.at[relay_index(v, h), j, h], g.at[v, t], rb_send.at[j, h], g_recv.at[v, t],
            twin * group + j, x * 2 + h,
        )

    def relay_step(v):
        for j, h in pairs:

            @pl.when(jnp.logical_and(near, jnp.logical_not(is_direct(v, h))))
            def _():
                to_relay(v, j, h).wait_recv()
                relay(v, j, h).start()

    def forward(v, ts):
        return remote(g.at[v, ts], g.at[v, ts], f_send.at[v, ts], g_recv.at[v, ts], t, twin)

    def got(v, ts):
        forward(v, ts).wait_recv()

    def pass_on(v, ts):
        got(v, ts)
        forward(v, ts).start()

    def arrivals(v):
        @pl.when(near)
        def _():
            @pl.when(jnp.logical_not(home))
            def _():
                got(v, t)

            def take_near(i):
                ts = near_source(i)
                got(v, ts)

                @pl.when(ts // group != t // group)
                def _():
                    forward(v, ts).start()

            loop(half_t, take_near, 1)

            @pl.when(is_direct(v, c))
            def _():
                loop(half_t, lambda i: pass_on(v, far_source(i)))

        @pl.when(jnp.logical_and(far, jnp.logical_not(is_direct(v, c))))
        def _():
            loop(half_t, lambda i: pass_on(v, far_source(i)))

    def second_hand(v):
        @pl.when(far)
        def _():
            loop(half_t, lambda i: got(v, near_source(i)))

            @pl.when(is_direct(v, c))
            def _():
                loop(half_t, lambda i: got(v, far_source(i)))

        @pl.when(jnp.logical_and(near, jnp.logical_not(is_direct(v, c))))
        def _():
            loop(half_t, lambda i: got(v, far_source(i)))

    def forwarded(v):
        def near_sent(i):
            @pl.when(near_source(i) // group != t // group)
            def _():
                forward(v, near_source(i)).wait_send()

        @pl.when(near)
        def _():
            loop(half_t, near_sent)

        @pl.when(near == is_direct(v, c))
        def _():
            loop(half_t, lambda i: forward(v, far_source(i)).wait_send())

    def to_mate(v, place):
        return remote(g.at[v], place, o_send.at[v], o_recv.at[v], t, mate)

    spare = units // 2

    def hand_to_mate(v):
        @pl.when(v < lead)
        def _():
            to_mate(v, first.at[v]).start()

        @pl.when(jnp.logical_and(v >= lead, v < spare))
        def _():
            to_mate(v, middle.at[v - lead]).start()

        @pl.when(v >= spare)
        def _():
            pl.semaphore_wait(credit, 1)
            to_mate(v, s.at[v - spare]).start()

    def give_credit(v):
        at = v - spare
        both = s.at[at, 0:2]
        for j, h in pairs:

            @pl.when(jnp.logical_not(stays(j, h)))
            def _():
                remote(both, both, s_send.at[at, j, h], o_recv.at[0], t, mate).wait_send()

            @pl.when(level)
            def _():
                remote(both, both, s_twin.at[at, j, h], o_recv.at[0], t, mate).wait_send()

        pl.semaphore_signal(
            credit, inc=1, device_id={"tensor": t, "dp": mate}, device_id_type=MESH
        )

    def merge_unit(v):
        k, q = v // per, lax.rem(v, per)
        lanes = pl.ds(pl.multiple_of(q * unit, unit), unit)
        second_hand(v)
        factor = right[k, :, lanes]
        squares = jnp.zeros((unit, 128), jnp.float32)
        for n in range(tensor_count):
            piece = g[v, n].astype(jnp.float32) + lax.dot_general(
                factor, left[n, k], (((0,), (0,)), ((), ())), preferred_element_type=jnp.float32
            )
            merged[:, n * rows : (n + 1) * rows] = piece
            for b in range(rows // 128):
                part = piece[:, b * 128 : (b + 1) * 128]
                squares = squares + part * part
        total = jnp.sum(squares, axis=1, keepdims=True)
        row = lax.broadcasted_iota(jnp.int32, (projections, unit), 0)
        chosen = jnp.zeros((1, unit), jnp.float32)
        for e in range(experts):
            line = strength[e, :, lanes].astype(jnp.float32)
            line = jnp.where(row + e * projections == k, line, 0.0)
            chosen = chosen + jnp.sum(line, axis=0, keepdims=True)
        wide = jnp.broadcast_to(chosen, (unit, unit)).T
        scaling = wide / jnp.sqrt(total + 1e-06)

        forwarded(v)
        for n in range(tensor_count):
            for b in range(rows // 128):
                at = slice(b * 128, (b + 1) * 128)
                wide_at = slice(n * rows + b * 128, n * rows + (b + 1) * 128)
                g[v, n, :, at] = (merged[:, wide_at] * scaling).astype(g.dtype)
        hand_to_mate(v)

    carrier = lax.rem(t, 2) == c

    def left_out(ts):
        return remote(lt, left.at[t], l_send.at[ts], l_recv.at[t], ts, d)

    def left_mate(ts):
        return remote(left.at[ts], left.at[ts], l_mate.at[ts], l_recv.at[ts], t, mate)

    def left_twin(ts):
        return remote(left.at[ts], left.at[ts], l_twin.at[ts], l_recv.at[ts], t, twin)

    own_left = pltpu.make_async_copy(lt, left.at[t], l_own)

    def factors(h, dp):
        at = pl.multiple_of(lax.rem(t, group) * serve + h * half, unit)
        way = dp // 2
        return (
            remote(r.at[:, :, pl.ds(at, half)], right, p_send.at[0, way, h], p_recv.at[0], t, dp),
            remote(m.at[:, :, pl.ds(at, half)], strength, p_send.at[1, way, h], p_recv.at[1], t, dp),
        )

    def own_factors(h):
        at = pl.multiple_of(lax.rem(t, group) * serve + h * half, unit)
        return (
            pltpu.make_async_copy(r.at[:, :, pl.ds(at, half)], right, p_recv.at[0]),
            pltpu.make_async_copy(m.at[:, :, pl.ds(at, half)], strength, p_recv.at[1]),
        )

    def each_factor(remote_do, own_do):
        for way in range(2):
            for h in range(2):
                dp = way * 2 + h

                if remote_do:

                    @pl.when(jnp.logical_and(home, d != dp))
                    def _():
                        for copy in factors(h, dp):
                            remote_do(copy)

                if own_do:

                    @pl.when(jnp.logical_and(home, d == dp))
                    def _():
                        for copy in own_factors(h):
                            own_do(copy)

    start_load(0)
    start_load(1)
    own_left.start()
    barrier = pltpu.get_barrier_semaphore()

    def greet(i):
        to, at = i // 4, lax.rem(i, 4)

        @pl.when(jnp.logical_or(to != t, at != d))
        def _():
            pl.semaphore_signal(
                barrier, inc=1, device_id={"tensor": to, "dp": at}, device_id_type=MESH
            )

    loop(4 * tensor_count, greet)
    pl.semaphore_wait(barrier, 4 * tensor_count - 1)

    @pl.when(carrier)
    def _():
        loop(half_t, lambda i: left_out(near_source(i)).start(), 1)

        @pl.when(far)
        def _():
            loop(half_t, lambda i: left_out(far_source(i)).start())

    each_factor(lambda copy: copy.start(), lambda copy: copy.start())

    def left_round(ts, target):
        return remote(left.at[ts], left.at[ts], l_twin.at[target], l_recv.at[ts], target, d)

    def carries(ts):
        return lax.rem(ts, 2) == c

    def spread(ts):
        @pl.when(carries(ts))
        def _():
            left_mate(ts).wait_recv()
            left_mate(ts).start()

    def take(ts):
        @pl.when(jnp.logical_not(carries(ts)))
        def _():
            left_mate(ts).wait_recv()

    opposite = far_source(0)

    def spread_first():
        loop(half_t, lambda i: spread(near_source(i)), 1)

        @pl.when(near)
        def _():
            loop(half_t, lambda i: spread(far_source(i)))

            @pl.when(carries(opposite))
            def _():
                left_twin(opposite).start()

    def spread_second():
        @pl.when(far)
        def _():
            spread(opposite)

            @pl.when(carries(opposite))
            def _():
                loop(half_t, lambda i: left_round(opposite, near_source(i)).start(), 1)

            loop(half_t, lambda i: spread(far_source(i)), 1)

    def take_factors():
        own_left.wait()
        loop(half_t, lambda i: take(near_source(i)), 1)
        loop(half_t, lambda i: take(far_source(i)))

        @pl.when(jnp.logical_not(home))
        def _():
            for copy in factors(0, mate):
                copy.wait_recv()

        each_factor(None, lambda copy: copy.wait())

    def step(u):
        @pl.when(u < units)
        def _():
            flip_and_send(u)

        v = u - RELAY_LAG

        @pl.when(jnp.logical_and(v >= 0, v < units))
        def _():
            relay_step(v)

        v = u - FORWARD_LAG

        @pl.when(jnp.logical_and(v >= 0, v < units))
        def _():
            arrivals(v)

        v = u - CREDIT_LAG

        @pl.when(jnp.logical_and(v >= spare, v < units))
        def _():
            give_credit(v)

        for at, what in enumerate((spread_first, spread_second, take_factors)):
            pl.when(u == FORWARD_LAG + at)(what)

        v = u - FORWARD_LAG - MERGE_LAG

        @pl.when(v >= 0)
        def _():
            merge_unit(v)

    loop(units + FORWARD_LAG + MERGE_LAG, step)

    def last(v):
        to_mate(v, g.at[v]).wait_send()
        to_mate(v, g.at[v]).wait_recv()

    loop(units, last)

    @pl.when(near)
    def _():
        for j, h in pairs:
            sent = rb.at[0 : units - (units + 1 + h) // 3, j, h]
            remote(sent, sent, rb_send.at[j, h], g_recv.at[0, 0], t, twin).wait_send()

    @pl.when(carrier)
    def _():
        loop(half_t, lambda i: left_out(near_source(i)).wait_send(), 1)

        @pl.when(far)
        def _():
            loop(half_t, lambda i: left_out(far_source(i)).wait_send())

    def left_sent(ts):
        @pl.when(carries(ts))
        def _():
            left_mate(ts).wait_send()

    loop(half_t, lambda i: left_sent(near_source(i)), 1)
    loop(half_t, lambda i: left_sent(far_source(i)))

    @pl.when(carries(opposite))
    def _():
        @pl.when(near)
        def _():
            left_twin(opposite).wait_send()

        @pl.when(far)
        def _():
            loop(half_t, lambda i: left_round(opposite, near_source(i)).wait_send(), 1)

    each_factor(lambda copy: copy.wait_send(), None)


def place_kernel(stacks, first, middle, last, own, o, held, stage, in_sem, out_sem):
    c = lax.rem(lax.axis_index("dp"), 2)
    units, count, unit, rows = own.shape
    half = o.shape[1] // 2
    per = units // stacks
    lead, kept = first.shape[0], middle.shape[0]
    depth = stage.shape[0]

    def fetch(v):
        return pltpu.make_async_copy(first.at[v], held.at[v], in_sem.at[v])

    def leave(slot, k, at):
        return pltpu.make_async_copy(stage.at[slot], o.at[k, at], out_sem.at[slot])

    def place(src, v, core, turn):
        k, q = v // per, lax.rem(v, per)
        at = pl.ds(pl.multiple_of(core * half + q * unit, unit), unit)
        slot = lax.rem(turn, depth)

        @pl.when(turn >= depth)
        def _():
            leave(slot, k, at).wait()

        for n in range(count):
            stage[slot, :, n * rows : (n + 1) * rows] = src[n]
        leave(slot, k, at).start()

    def loop(begin, end, body):
        lax.fori_loop(begin, end, lambda v, carry: (body(v), carry)[1], 0)

    def from_hbm(v):
        fetch(v).wait()
        place(held.at[v], v, 1 - c, units + v)

    loop(0, lead, lambda v: fetch(v).start())
    loop(0, units, lambda v: place(own.at[v], v, c, v))
    loop(0, lead, from_hbm)
    loop(lead, lead + kept, lambda v: place(middle.at[v - lead], v, 1 - c, units + v))
    loop(lead + kept, units, lambda v: place(last.at[v - lead - kept], v, 1 - c, units + v))
    for slot in range(depth):
        leave(slot, 0, pl.ds(0, unit)).wait()


def fused(w, lt, r, m, tensor_count):
    stacks, rows, cols = w.shape
    rank = lt.shape[1]
    group = tensor_count // 4
    serve = cols // group
    half = serve // 2
    per = half // UNIT
    units = stacks * per
    relayed = units - (units + 1) // 3
    dma = pltpu.SemaphoreType.DMA
    hbm = pl.BlockSpec(memory_space=pl.ANY)
    width = tensor_count * rows
    vmem = pl.BlockSpec(memory_space=pltpu.VMEM)
    spare = units // 2
    lead = max(1, spare - KEPT)
    block = (tensor_count, UNIT, rows)
    parts = pl.pallas_call(
        functools.partial(fused_kernel, tensor_count, lead),
        out_shape=(
            jax.ShapeDtypeStruct((lead, *block), w.dtype),
            pltpu.VMEM((spare - lead, *block), w.dtype),
            pltpu.VMEM((spare, *block), w.dtype),
            pltpu.VMEM((units, *block), w.dtype),
        ),
        in_specs=[hbm] * 4,
        out_specs=(hbm, vmem, vmem, vmem),
        scratch_shapes=[
            pltpu.VMEM((relayed, group, 2, UNIT, rows), w.dtype),
            pltpu.VMEM((2, group, 2, rows, UNIT), w.dtype),
            pltpu.VMEM((tensor_count, stacks, rank, rows), w.dtype),
            pltpu.VMEM((stacks, rank, half), w.dtype),
            pltpu.VMEM((*m.shape[:2], half), m.dtype),
            pltpu.VMEM((UNIT, width), jnp.float32),
            dma((2, group, 2)),
            dma((spare, group, 2)),
            dma((spare, group, 2)),
            dma((units, tensor_count)),
            dma((relayed, group, 2)),
            dma((group, 2)),
            dma((units, tensor_count)),
            dma,
            dma((tensor_count,)),
            dma((tensor_count,)),
            dma((tensor_count,)),
            dma((tensor_count,)),
            dma((2,)),
            dma((2, 2, 2)),
            dma((units,)),
            dma((units,)),
            pltpu.SemaphoreType.REGULAR,
        ],
        compiler_params=pltpu.CompilerParams(
            collective_id=0, has_side_effects=True, vmem_limit_bytes=14_200_000
        ),
    )(w, lt, r, m)
    return pl.pallas_call(
        functools.partial(place_kernel, stacks),
        out_shape=jax.ShapeDtypeStruct((stacks, serve, width), w.dtype),
        in_specs=[hbm, vmem, vmem, vmem],
        out_specs=hbm,
        scratch_shapes=[
            pltpu.VMEM((lead, *block), w.dtype),
            pltpu.VMEM((STAGED, UNIT, width), w.dtype),
            dma((lead,)),
            dma((STAGED,)),
        ],
        compiler_params=pltpu.CompilerParams(vmem_limit_bytes=13_500_000),
    )(parts[0], *(pltpu.with_memory_space_constraint(p, pltpu.VMEM) for p in parts[1:]))


def fits(tensor_count, replica_count, stacks, rows, cols):
    if replica_count != 4 or tensor_count % 8 or cols % (tensor_count // 2 * UNIT) or rows % 128:
        return False
    units = stacks * (cols // (tensor_count // 2 * UNIT))
    pieces = units * tensor_count * UNIT * rows
    return units % 2 == 0 and units // 2 > KEPT and pieces <= 15_000_000


def shards(base_weight, adapter_left, adapter_right, magnitude):
    tensor_count = lax.axis_size("tensor")
    replica_count = lax.axis_size("dp")
    experts, projections, rows, cols = base_weight.shape
    rank = adapter_left.shape[3]
    stacks = experts * projections
    group = tensor_count // replica_count
    serve = cols // group
    chunks = stacks if tensor_count <= 16 else 1
    relayed = (2 * (serve // 16) + 1) // 3 * 16

    if fits(tensor_count, replica_count, stacks, rows, cols):
        out = fused(
            base_weight.reshape(stacks, rows, cols),
            adapter_left.swapaxes(2, 3).reshape(stacks, rank, rows),
            adapter_right.reshape(stacks, rank, cols),
            magnitude,
            tensor_count,
        )
        return out.reshape(experts, projections, serve, -1)
    s = flip(base_weight.reshape(stacks, rows, cols))
    if chunks == 1:
        s = s.reshape(1, stacks, group, serve, rows).swapaxes(1, 2)
    else:
        s = s.reshape(chunks, group, 1, serve, rows)
    g = exchange(s, tensor_count, replica_count, relayed).reshape(tensor_count, stacks, serve, rows)

    left = lax.all_gather(adapter_left.swapaxes(2, 3), "tensor", axis=3, tiled=True)
    right_all = lax.all_gather(adapter_right, "dp", axis=3, tiled=True)
    magnitude_all = lax.all_gather(magnitude, "dp", axis=2, tiled=True)
    start = lax.axis_index("tensor") * serve
    right = lax.dynamic_slice_in_dim(right_all, start, serve, 3).swapaxes(2, 3)
    strength = lax.dynamic_slice_in_dim(magnitude_all, start, serve, 2)
    out = merge(
        g,
        left.reshape(stacks, rank, -1),
        right.reshape(stacks, serve, rank),
        strength.reshape(stacks, serve, 1),
    )
    return out.reshape(experts, projections, serve, -1)


def solution(mesh):
    in_specs = (
        P(None, None, "tensor", "dp"),
        P(None, None, "tensor", None),
        P(None, None, None, "dp"),
        P(None, None, "dp"),
    )
    out_specs = P(None, None, "tensor", None)
    return jax.shard_map(shards, mesh=mesh, in_specs=in_specs, out_specs=out_specs, check_vma=False)
```
